16 devices in a mesh: fsdp: 2 (over z), ep: 8 (over y, x, core).
Axes of the slice: x: 2, y: 2, z: 2, core: 2. Of those that a mesh axis runs over, the one named last changes fastest.
Arguments:
- x_tok: bfloat16 [32768, 512], P(('fsdp', 'ep'))
- dy_tok: bfloat16 [32768, 512], P(('fsdp', 'ep'))
- expert_ids: int32 [32768, 6], P(('fsdp', 'ep'))
- route_w: float32 [32768, 6], P(('fsdp', 'ep'))
- w_gate: bfloat16 [160, 512, 384], P('ep', 'fsdp')
- w_up: bfloat16 [160, 512, 384], P('ep', 'fsdp')
- w_down: bfloat16 [160, 384, 512], P('ep', None, 'fsdp')
Outputs:
- output 1: bfloat16 [32768, 512], P(('fsdp', 'ep'))
- output 2: float32 [32768, 6], P(('fsdp', 'ep'))
- output 3: float32 [160, 512, 384], P('ep', 'fsdp')
- output 4: float32 [160, 512, 384], P('ep', 'fsdp')
- output 5: float32 [160, 384, 512], P('ep', None, 'fsdp')
All inputs are finite; a program needn't handle non-finite values.
Results may differ from the reference program's by a relative error of at most 0.00867669.
Values are sent between devices in bfloat16 or wider.
A program may use at most 1 GiB of HBM per device.

```python
import jax
import jax.numpy as jnp
from jax import lax

D_MODEL = 512
D_FF = 384
EXPERTS = 160
TOP_K = 6
TOK_DEV = 2048
DEVICES = 16
CAPACITY = 232

TOKENS = DEVICES * TOK_DEV
SLOTS = EXPERTS * CAPACITY
HOT_COUNT = max(1, TOP_K // 2)


def draw_routing(root_key):
    key_hot, key_score = jax.random.split(root_key)
    hot_rank = jax.random.permutation(key_hot, EXPERTS)
    bias = jnp.where(hot_rank < HOT_COUNT, 768, 0).astype(jnp.int32)
    expert_col = jnp.arange(EXPERTS, dtype=jnp.int32)

    def one_device(dev_key):
        noise = jax.random.randint(dev_key, (TOK_DEV, EXPERTS), 0, 1024, dtype=jnp.int32)
        score = (noise + bias[None, :]) * EXPERTS + expert_col[None, :]
        return lax.top_k(score, TOP_K)[1]

    chosen = lax.map(one_device, jax.random.split(key_score, DEVICES))
    return chosen.reshape(TOKENS, TOP_K).astype(jnp.int32)


def setup_inputs(seed: int = 0) -> dict:
    key_list = jax.random.split(jax.random.key(seed), 7)
    x_tok = jax.random.normal(key_list[0], (TOKENS, D_MODEL), jnp.float32)
    dy_tok = jax.random.normal(key_list[1], (TOKENS, D_MODEL), jnp.float32)
    expert_ids = draw_routing(key_list[2])
    route_w = jax.random.uniform(key_list[3], (TOKENS, TOP_K), jnp.float32, 0.1, 1.0)
    w_gate = jax.random.normal(key_list[4], (EXPERTS, D_MODEL, D_FF), jnp.float32) * D_MODEL ** -0.5
    w_up = jax.random.normal(key_list[5], (EXPERTS, D_MODEL, D_FF), jnp.float32) * D_MODEL ** -0.5
    w_down = jax.random.normal(key_list[6], (EXPERTS, D_FF, D_MODEL), jnp.float32) * D_FF ** -0.5
    return {
        "x_tok": x_tok.astype(jnp.bfloat16),
        "dy_tok": dy_tok.astype(jnp.bfloat16),
        "expert_ids": expert_ids,
        "route_w": route_w,
        "w_gate": w_gate.astype(jnp.bfloat16),
        "w_up": w_up.astype(jnp.bfloat16),
        "w_down": w_down.astype(jnp.bfloat16),
    }


def slot_positions(ids_dev):
    onehot = (ids_dev[:, None] == jnp.arange(EXPERTS, dtype=jnp.int32)[None, :]).astype(jnp.int32)
    before = jnp.cumsum(onehot, axis=0) - onehot
    position = jnp.sum(before * onehot, axis=1)
    return jnp.where(position < CAPACITY, ids_dev * CAPACITY + position, SLOTS)


def swiglu_grads(pre_gate, pre_up, grad_hidden):
    sigma = jax.nn.sigmoid(pre_gate)
    grad_gate = grad_hidden * pre_up * sigma * (1.0 + pre_gate * (1.0 - sigma))
    grad_up = grad_hidden * pre_gate * sigma
    return grad_gate.astype(jnp.bfloat16), grad_up.astype(jnp.bfloat16)


def reference(x_tok, dy_tok, expert_ids, route_w, w_gate, w_up, w_down):
    dest_slot = lax.map(slot_positions, expert_ids.reshape(DEVICES, TOK_DEV * TOP_K))
    pair_ids = jnp.arange(TOKENS * TOP_K, dtype=jnp.int32).reshape(DEVICES, TOK_DEV * TOP_K)
    dev_rows = jnp.broadcast_to(jnp.arange(DEVICES, dtype=jnp.int32)[:, None], dest_slot.shape)
    slot_src = jnp.full((DEVICES, SLOTS + 1), TOKENS * TOP_K, jnp.int32)
    slot_src = slot_src.at[dev_rows, dest_slot].set(pair_ids)[:, :SLOTS]
    per_expert = slot_src.reshape(DEVICES, EXPERTS, CAPACITY).transpose(1, 0, 2).reshape(EXPERTS, DEVICES * CAPACITY)
    route_flat = route_w.reshape(-1)

    def expert_step(carry, step_in):
        dx_acc, dr_acc = carry
        pair_src, w_gate_e, w_up_e, w_down_e = step_in
        tok_rows = pair_src // TOP_K
        x_rows = jnp.take(x_tok, tok_rows, axis=0, mode="fill", fill_value=0)
        dy_rows = jnp.take(dy_tok, tok_rows, axis=0, mode="fill", fill_value=0)
        gate_rows = jnp.take(route_flat, pair_src, axis=0, mode="fill", fill_value=0)
        pre_gate = jnp.dot(x_rows, w_gate_e, preferred_element_type=jnp.float32)
        pre_up = jnp.dot(x_rows, w_up_e, preferred_element_type=jnp.float32)
        hidden = (jax.nn.silu(pre_gate) * pre_up).astype(jnp.bfloat16)
        y_rows = jnp.dot(hidden, w_down_e, preferred_element_type=jnp.float32)
        dy_wide = dy_rows.astype(jnp.float32)
        scaled_dy = (gate_rows[:, None] * dy_wide).astype(jnp.bfloat16)
        dr_rows = jnp.sum(dy_wide * y_rows, axis=1)
        grad_hidden = jnp.dot(scaled_dy, w_down_e.T, preferred_element_type=jnp.float32)
        grad_gate, grad_up = swiglu_grads(pre_gate, pre_up, grad_hidden)
        dx_rows = (jnp.dot(grad_gate, w_gate_e.T, preferred_element_type=jnp.float32)
                   + jnp.dot(grad_up, w_up_e.T, preferred_element_type=jnp.float32)).astype(jnp.bfloat16)
        dw_gate = jnp.dot(x_rows.T, grad_gate, preferred_element_type=jnp.float32)
        dw_up = jnp.dot(x_rows.T, grad_up, preferred_element_type=jnp.float32)
        dw_down = jnp.dot(hidden.T, scaled_dy, preferred_element_type=jnp.float32)
        dx_acc = dx_acc.at[tok_rows].add(dx_rows.astype(jnp.float32), mode="drop")
        dr_acc = dr_acc.at[pair_src].set(dr_rows, mode="drop")
        return (dx_acc, dr_acc), (dw_gate, dw_up, dw_down)

    init = (jnp.zeros((TOKENS, D_MODEL), jnp.float32), jnp.zeros((TOKENS * TOP_K,), jnp.float32))
    (dx_acc, dr_acc), (grad_w_gate, grad_w_up, grad_w_down) = lax.scan(
        expert_step, init, (per_expert, w_gate, w_up, w_down))
    grad_x = dx_acc.astype(jnp.bfloat16)
    route_w_grad = dr_acc.reshape(TOKENS, TOP_K)
    return (grad_x, route_w_grad, grad_w_gate, grad_w_up, grad_w_down)
```

```python
import functools

import jax
import jax.numpy as jnp
from jax import lax
from jax.experimental import pallas as pl
from jax.experimental.pallas import tpu as pltpu
from jax.sharding import PartitionSpec as P

CAP_FACTOR = 3
SUB = 16
BLK = 256
META = 128
F32 = jnp.float32
BF16 = jnp.bfloat16


def capacity_of(tok_dev, top_k, experts):
    return max(8, ((CAP_FACTOR * tok_dev * top_k // experts + 7) // 8) * 8)


def split3(v):
    hi = lax.reduce_precision(v, 8, 7)
    mid = lax.reduce_precision(v - hi, 8, 7)
    return hi, mid, v - hi - mid


def build_onehot(oh_ref, pos_ref, subexp, sublocal, first_sub):
    n_tok = oh_ref.shape[1]
    row_iota = lax.broadcasted_iota(jnp.int32, (SUB, n_tok), 0)
    for sub in range(BLK // SUB):
        q = first_sub + sub
        row = pos_ref[0, pl.ds(subexp[q], 1), :]
        hit = row_iota == (row - sublocal[q])
        oh_ref[sub * SUB:(sub + 1) * SUB, :] = jnp.where(hit, 1.0, 0.0).astype(BF16)


def gather_kernel(nsub_max, base, nblk, subexp, sublocal, subdst, half, xo, xp, do, dp, meta, pos, *rest):
    g_out, oh, buf, sem = rest[-4:]
    s = pl.program_id(0)
    k = base + s
    n = nblk[k]

    def wait(slot):
        pltpu.make_async_copy(buf.at[slot], g_out.at[pl.ds(0, BLK)], sem.at[slot]).wait()

    def block(b, _):
        slot = lax.rem(b, 2)
        first = k * nsub_max + b * (BLK // SUB)
        build_onehot(oh, pos, subexp, sublocal, first)

        @pl.when(b >= 2)
        def _():
            wait(slot)

        col = 0
        for ref in (xo, xp, do, dp, meta):
            w = ref.shape[1]
            buf[slot, :, col:col + w] = jnp.dot(oh[...], ref[...], preferred_element_type=F32).astype(BF16)
            col += w
        for sub in range(BLK // SUB):
            dst = pl.multiple_of(subdst[first + sub], SUB)
            pltpu.make_async_copy(buf.at[slot, pl.ds(sub * SUB, SUB)], g_out.at[pl.ds(dst, SUB)], sem.at[slot]).start()
        return 0

    lax.fori_loop(0, n, block, 0)

    @pl.when(n >= 1)
    def _():
        wait(lax.rem(n + 1, 2))

    @pl.when(n >= 2)
    def _():
        wait(lax.rem(n, 2))


def gather_call(base, tables, x_all, dy_all, meta_all, pos_all, rows, g_prev):
    nblk, subexp, sublocal, subdst, half = tables
    n_src = pos_all.shape[0]
    n_tok = pos_all.shape[2]
    nsub_max = subexp.shape[0] // nblk.shape[0]
    dh = x_all.shape[1] // 2
    width = 4 * dh + META
    own = pl.BlockSpec((n_tok, dh), lambda s, *t: (s, t[4][0]))
    oth = pl.BlockSpec((n_tok, dh), lambda s, *t: (s, 1 - t[4][0]))
    in_specs = [own, oth, own, oth,
                pl.BlockSpec((n_tok, META), lambda s, *t: (s, 0)),
                pl.BlockSpec((1,) + pos_all.shape[1:], lambda s, *t: (s, 0, 0))]
    args = [x_all, x_all, dy_all, dy_all, meta_all, pos_all]
    alias = {}
    if g_prev is not None:
        in_specs.append(pl.BlockSpec(memory_space=pl.ANY))
        args.append(g_prev)
        alias = {11: 0}
    return pl.pallas_call(
        functools.partial(gather_kernel, nsub_max, base),
        out_shape=jax.ShapeDtypeStruct((rows, width), BF16),
        grid_spec=pltpu.PrefetchScalarGridSpec(
            num_scalar_prefetch=5, grid=(n_src,), in_specs=in_specs,
            out_specs=pl.BlockSpec(memory_space=pl.ANY),
            scratch_shapes=[pltpu.VMEM((BLK, n_tok), BF16), pltpu.VMEM((2, BLK, width), BF16),
                            pltpu.SemaphoreType.DMA((2,))]),
        input_output_aliases=alias,
        cost_estimate=pl.CostEstimate(flops=int(40e9), bytes_accessed=int(60e6), transcendentals=0),
        name="gather_rows",
    )(nblk, subexp, sublocal, subdst, half, *args)


def nt_dot(a, b):
    return lax.dot_general(a, b, (((1,), (1,)), ((), ())), preferred_element_type=F32)


def tn_dot(a, b):
    return lax.dot_general(a, b, (((0,), (0,)), ((), ())), preferred_element_type=F32)


def expert_kernel(blk_end, exp_rows, first_expert, g_hbm, w1o, w1p, w3o, w3p, w2o, w2p, dx_hbm, dw1, dw3, dw2,
                  w13, w2, gbuf, dxbuf, gsem, dxsem):
    e = pl.program_id(0)
    dh = w1o.shape[1]
    d = 2 * dh
    f = w1o.shape[2]
    last = pl.num_programs(0) - 1
    total = blk_end[last]
    begin = jnp.where(e == 0, 0, blk_end[jnp.maximum(e - 1, 0)])
    end = blk_end[e]

    def fetch(b):
        src = pl.multiple_of(b * BLK, BLK)
        slot = lax.rem(b, 2)
        return pltpu.make_async_copy(g_hbm.at[pl.ds(src, BLK)], gbuf.at[slot], gsem.at[slot])

    def store(b):
        dst = pl.multiple_of(b * BLK, BLK)
        slot = lax.rem(b, 2)
        return pltpu.make_async_copy(dxbuf.at[slot], dx_hbm.at[pl.ds(dst, BLK)], dxsem.at[slot])

    @pl.when(e == 0)
    def _():
        fetch(0).start()

    w13[0:dh, 0:f] = w1o[0]
    w13[dh:d, 0:f] = w1p[0]
    w13[0:dh, f:2 * f] = w3o[0]
    w13[dh:d, f:2 * f] = w3p[0]
    w2[:, 0:dh] = w2o[0]
    w2[:, dh:d] = w2p[0]
    dw1[...] = jnp.zeros_like(dw1)
    dw3[...] = jnp.zeros_like(dw3)
    dw2[...] = jnp.zeros_like(dw2)

    def block(b, _):
        slot = lax.rem(b, 2)

        @pl.when(b + 1 < total)
        def _():
            fetch(b + 1).start()

        fetch(b).wait()

        @pl.when(b >= 2)
        def _():
            store(b - 2).wait()

        g = gbuf.at[slot]
        dx = dxbuf.at[slot]
        cnt = exp_rows[e] - (b - begin) * BLK

        def masked(v):
            keep = lax.broadcasted_iota(jnp.int32, v.shape, 0) < cnt
            return jnp.where(keep, v, jnp.zeros_like(v))

        x = masked(g[:, 0:d])
        dy = masked(g[:, d:2 * d])
        meta = masked(g[:, 2 * d:2 * d + META].astype(F32))
        lane = lax.broadcasted_iota(jnp.int32, meta.shape, 1)
        ids = pltpu.roll(meta, META - 32, 1)
        mine = (ids == (first_expert[0] + e).astype(F32)) & (lane < 24)

        def piece(c):
            return jnp.sum(jnp.where(mine & (lane >= 8 * c) & (lane < 8 * c + 8), meta, 0.0), axis=1, keepdims=True)

        r = piece(0) + piece(1) + piece(2)
        dy32 = dy.astype(F32)
        scaled = (r * dy32).astype(BF16)
        h = jnp.dot(x, w13[...], preferred_element_type=F32)
        h1 = h[:, :f]
        h3 = h[:, f:]
        sig = jax.nn.sigmoid(h1)
        act = ((h1 * sig) * h3).astype(BF16)
        y = jnp.dot(act, w2[:, 0:dh], preferred_element_type=F32)
        dr = jnp.sum(dy32[:, 0:dh] * y, axis=1, keepdims=True)
        da = nt_dot(scaled, w2[...])
        dh1 = (da * h3 * sig * (1.0 + h1 * (1.0 - sig))).astype(BF16)
        dh3 = (da * h1 * sig).astype(BF16)
        dx[:, 0:dh] = (nt_dot(dh1, w1o[0]) + nt_dot(dh3, w3o[0])).astype(BF16)
        hi = dr.astype(BF16).astype(F32)
        mid = (dr - hi).astype(BF16).astype(F32)
        lo = dr - hi - mid
        spread = jnp.where(lane < 8, hi, jnp.where(lane < 16, mid, lo))
        dx[:, dh:dh + META] = jnp.where(mine, spread, 0.0).astype(BF16)
        store(b).start()
        dw1[0] += tn_dot(x[:, 0:dh], dh1)
        dw3[0] += tn_dot(x[:, 0:dh], dh3)
        dw2[0] += tn_dot(act, scaled[:, 0:dh])
        return 0

    lax.fori_loop(begin, end, block, 0)

    @pl.when(e == last)
    def _():
        store(total - 1).wait()
        store(total - 2).wait()


def expert_call(blk_end, exp_rows, first_expert, g, w_own, w_oth, rows):
    e, dh, f = w_own[0].shape
    width = g.shape[1]
    wspec = pl.BlockSpec((1, dh, f), lambda e, *t: (e, 0, 0))
    dspec = pl.BlockSpec((1, f, dh), lambda e, *t: (e, 0, 0))
    hbm = pl.BlockSpec(memory_space=pl.ANY)
    return pl.pallas_call(
        expert_kernel,
        out_shape=(jax.ShapeDtypeStruct((rows, dh + META), BF16),
                   jax.ShapeDtypeStruct((e, dh, f), F32), jax.ShapeDtypeStruct((e, dh, f), F32),
                   jax.ShapeDtypeStruct((e, f, dh), F32)),
        grid_spec=pltpu.PrefetchScalarGridSpec(
            num_scalar_prefetch=3, grid=(e,),
            in_specs=[hbm, wspec, wspec, wspec, wspec, dspec, dspec],
            out_specs=[hbm, wspec, wspec, dspec],
            scratch_shapes=[pltpu.VMEM((2 * dh, 2 * f), BF16), pltpu.VMEM((f, 2 * dh), BF16),
                            pltpu.VMEM((2, BLK, width), BF16), pltpu.VMEM((2, BLK, dh + META), BF16),
                            pltpu.SemaphoreType.DMA((2,)), pltpu.SemaphoreType.DMA((2,))]),
        cost_estimate=pl.CostEstimate(flops=int(60e9), bytes_accessed=int(120e6), transcendentals=0),
        name="expert_backward",
    )(blk_end, exp_rows, first_expert, g, w_own[0], w_oth[0], w_own[1], w_oth[1], w_own[2], w_oth[2])


def scatter_kernel(nsub_max, base, dh, nblk, subexp, sublocal, subsrc, pos, dx_hbm, out, oh, buf, dracc, sem):
    s = pl.program_id(0)
    k = base + s
    n = nblk[k]
    out[...] = jnp.zeros_like(out)
    dracc[...] = jnp.zeros_like(dracc)

    def fetch(b, slot):
        first = k * nsub_max + b * (BLK // SUB)
        for sub in range(BLK // SUB):
            src = pl.multiple_of(subsrc[first + sub], SUB)
            pltpu.make_async_copy(dx_hbm.at[pl.ds(src, SUB)], buf.at[slot, pl.ds(sub * SUB, SUB)], sem.at[slot]).start()

    @pl.when(n >= 1)
    def _():
        fetch(0, 0)

    def block(b, _):
        slot = lax.rem(b, 2)

        @pl.when(b + 1 < n)
        def _():
            fetch(b + 1, 1 - slot)

        build_onehot(oh, pos, subexp, sublocal, k * nsub_max + b * (BLK // SUB))
        pltpu.make_async_copy(dx_hbm.at[pl.ds(0, BLK)], buf.at[slot], sem.at[slot]).wait()
        out[0, 0:dh, :] += tn_dot(buf[slot, :, 0:dh], oh[...])
        dracc[...] += tn_dot(buf[slot, :, dh:dh + META], oh[...])
        return 0

    lax.fori_loop(0, n, block, 0)
    out[0, dh:dh + 8, :] = dracc[0:8, :] + dracc[8:16, :] + dracc[16:24, :]


def scatter_call(base, nblk, subexp, sublocal, subsrc, pos_all, dx_rows):
    n_src, _, n_tok = pos_all.shape
    dh = dx_rows.shape[1] - META
    nsub_max = subexp.shape[0] // nblk.shape[0]
    return pl.pallas_call(
        functools.partial(scatter_kernel, nsub_max, base, dh),
        out_shape=jax.ShapeDtypeStruct((n_src, dh + 8, n_tok), F32),
        grid_spec=pltpu.PrefetchScalarGridSpec(
            num_scalar_prefetch=4, grid=(n_src,),
            in_specs=[pl.BlockSpec((1,) + pos_all.shape[1:], lambda s, *t: (s, 0, 0)),
                      pl.BlockSpec(memory_space=pl.ANY)],
            out_specs=pl.BlockSpec((1, dh + 8, n_tok), lambda s, *t: (s, 0, 0)),
            scratch_shapes=[pltpu.VMEM((BLK, n_tok), BF16), pltpu.VMEM((2, BLK, dh + META), BF16),
                            pltpu.VMEM((META, n_tok), F32), pltpu.SemaphoreType.DMA((2,))]),
        cost_estimate=pl.CostEstimate(flops=int(10e9), bytes_accessed=int(30e6), transcendentals=0),
        name="scatter_rows",
    )(nblk, subexp, sublocal, subsrc, pos_all, dx_rows)


def routing_tables(ids, first_expert, n_exp, capacity):
    n_src, _, n_tok = ids.shape
    eid = first_expert.astype(F32) + jnp.arange(n_exp, dtype=F32)
    mask = jnp.any(ids[:, None, :, :] == eid[None, :, None, None], axis=2)
    upper = (jnp.arange(n_tok)[:, None] < jnp.arange(n_tok)[None, :]).astype(BF16)
    before = jnp.dot(mask.reshape(n_src * n_exp, n_tok).astype(BF16), upper, preferred_element_type=F32)
    before = before.reshape(n_src, n_exp, n_tok)
    kept = mask & (before < capacity)
    pos = jnp.where(kept, before, -1.0).astype(jnp.int32)
    pos = jnp.pad(pos, ((0, 0), (0, (-n_exp) % 8), (0, 0)), constant_values=-1)
    cnt = jnp.sum(kept.astype(jnp.int32), axis=2)
    subs = (cnt + SUB - 1) // SUB
    cap_subs = -(-capacity // SUB)
    nsub_max = -(-n_exp * cap_subs // (BLK // SUB)) * (BLK // SUB)
    src_end = jnp.cumsum(subs, axis=1)
    src_off = src_end - subs
    nsub = src_end[:, -1]
    exp_subs = jnp.sum(subs, axis=0)
    exp_blocks = jnp.maximum(1, -(-exp_subs // (BLK // SUB)))
    blk_end = jnp.cumsum(exp_blocks)
    blk_off = blk_end - exp_blocks
    seg_off = blk_off[None, :] * (BLK // SUB) + jnp.cumsum(subs, axis=0) - subs
    q = jnp.arange(nsub_max, dtype=jnp.int32)
    subexp = jnp.minimum(jnp.sum((src_end[:, None, :] <= q[None, :, None]).astype(jnp.int32), axis=2), n_exp - 1)
    pick = subexp[:, :, None] == jnp.arange(n_exp)[None, None, :]
    rel = q[None, :] - jnp.sum(jnp.where(pick, src_off[:, None, :], 0), axis=2)
    live = q[None, :] < nsub[:, None]
    sublocal = jnp.where(live, rel * SUB, 1 << 20)
    seg = jnp.sum(jnp.where(pick, seg_off[:, None, :], 0), axis=2) + rel
    max_blocks = n_exp * max(1, -(-n_src * cap_subs // (BLK // SUB)))
    rows = max_blocks * BLK
    spare = rows + (q % (BLK // SUB))[None, :] * SUB
    subdst = jnp.where(live, seg * SUB, spare)
    subsrc = jnp.where(live, seg * SUB, 0)
    nblk = -(-nsub // (BLK // SUB))
    return (pos, nblk, subexp.reshape(-1), sublocal.reshape(-1), subdst.reshape(-1), subsrc.reshape(-1),
            blk_end, exp_subs * SUB, rows)


def solution(mesh):
    n_ep = mesh.shape["ep"]
    tok_spec = P(("fsdp", "ep"), None)
    spec_in = P("ep", "fsdp", None)
    spec_out = P("ep", None, "fsdp")
    swap = [(0, 1), (1, 0)]

    def per_device(x_tok, dy_tok, expert_ids, route_w, w_gate, w_up, w_down):
        tok_dev, top_k = expert_ids.shape
        exp_local = w_gate.shape[0]
        dh = w_gate.shape[1]
        capacity = capacity_of(tok_dev, top_k, exp_local * n_ep)
        me = lax.axis_index("fsdp")
        pad = ((0, 8 - top_k), (0, 0))
        info = jnp.stack([jnp.pad(expert_ids.T.astype(F32), pad, constant_values=-1.0),
                          jnp.pad(route_w.T, pad)])
        info = lax.all_gather(info, ("fsdp", "ep"), axis=0, tiled=False)
        info = info.reshape(2, n_ep, 2, 8, tok_dev)
        x_z = lax.ppermute(x_tok, "fsdp", swap)
        dy_z = lax.ppermute(dy_tok, "fsdp", swap)
        w_own = (w_gate, w_up, w_down)
        w_oth = tuple(lax.ppermute(w, "fsdp", swap) for w in w_own)
        x_a = lax.all_gather(x_tok, "ep", axis=0, tiled=True)
        dy_a = lax.all_gather(dy_tok, "ep", axis=0, tiled=True)
        x_b = lax.all_gather(x_z, "ep", axis=0, tiled=True)
        dy_b = lax.all_gather(dy_z, "ep", axis=0, tiled=True)

        info = jnp.where(me == 0, info, info[::-1]).reshape(2 * n_ep, 2, 8, tok_dev)
        ids = info[:, 0]
        first_expert = lax.axis_index("ep") * exp_local
        (pos, nblk, subexp, sublocal, subdst, subsrc, blk_end, exp_rows, rows) = routing_tables(
            ids, first_expert, exp_local, capacity)
        hi, mid, lo = split3(info[:, 1])
        none = jnp.zeros_like(hi)
        meta = jnp.concatenate([hi, mid, lo, none, ids, ids, ids] + [none] * 9, axis=1)
        meta = meta.astype(BF16).transpose(0, 2, 1).reshape(2, n_ep * tok_dev, META)
        half = me.reshape(1)
        tables = (nblk, subexp, sublocal, subdst, half)
        g = gather_call(0, tables, x_a, dy_a, meta[0], pos[:n_ep], rows + BLK, None)
        g = gather_call(n_ep, tables, x_b, dy_b, meta[1], pos[n_ep:], rows + BLK, g)
        dx_rows, dw_gate, dw_up, dw_down = expert_call(
            blk_end, exp_rows, first_expert.reshape(1), g, w_own, w_oth, rows)
        out_a = scatter_call(0, nblk, subexp, sublocal, subsrc, pos[:n_ep], dx_rows)
        out_b = scatter_call(n_ep, nblk, subexp, sublocal, subsrc, pos[n_ep:], dx_rows)
        sum_b = lax.psum_scatter(out_b, "ep", scatter_dimension=0, tiled=False)
        sum_a = lax.psum_scatter(out_a, "ep", scatter_dimension=0, tiled=False)
        dx_other = lax.ppermute(sum_b[:dh].astype(BF16), "fsdp", swap)
        dr_other = lax.ppermute(sum_b[dh:], "fsdp", swap)
        dx_mine = sum_a[:dh].astype(BF16)
        grad_x = jnp.where(me == 0, jnp.concatenate([dx_mine, dx_other]), jnp.concatenate([dx_other, dx_mine])).T
        route_grad = (sum_a[dh:] + dr_other)[:top_k].T
        return grad_x, route_grad, dw_gate, dw_up, dw_down

    return jax.shard_map(
        per_device, mesh=mesh,
        in_specs=(tok_spec, tok_spec, tok_spec, tok_spec, spec_in, spec_in, spec_out),
        out_specs=(tok_spec, tok_spec, spec_in, spec_in, spec_out),
        check_vma=False)
```

```python
import functools

import jax
import jax.numpy as jnp
from jax import lax
from jax.experimental import pallas as pl
from jax.experimental.pallas import tpu as pltpu
from jax.sharding import PartitionSpec as P


CAP_FACTOR = 3
SUB = 16
SRC_BLK = 384
EXP_BLK = 480
META = 128
F32 = jnp.float32
BF16 = jnp.bfloat16
HBM = pl.BlockSpec(memory_space=pl.ANY)


def capacity_of(tok_dev, top_k, experts):
    return max(8, ((CAP_FACTOR * tok_dev * top_k // experts + 7) // 8) * 8)


def nt_dot(a, b):
    return lax.dot_general(a, b, (((1,), (1,)), ((), ())), preferred_element_type=F32)


def tn_dot(a, b):
    return lax.dot_general(a, b, (((0,), (0,)), ((), ())), preferred_element_type=F32)


def build_onehot(oh_ref, pos_ref, subexp, sublocal, first_sub):
    n_tok = oh_ref.shape[1]
    one = jnp.ones((SUB, n_tok), BF16)
    for sub in range(SRC_BLK // SUB):
        q = first_sub + sub
        rows = pos_ref[0, pl.ds(pl.multiple_of(subexp[q] * SUB, SUB), SUB), :]
        want = jnp.full((SUB, n_tok), sublocal[q].astype(F32), F32).astype(BF16)
        oh_ref[sub * SUB:(sub + 1) * SUB, :] = jnp.where(rows == want, one, jnp.zeros_like(one))


def gather_kernel(nsub_max, with_meta, nblk, blk_before, subexp, sublocal, subdst, half, own, oth, info, pos, g_out, oh,
                  meta, buf, sem):
    k = pl.program_id(0)
    last = pl.num_programs(0) - 1
    n = nblk[k]
    done = blk_before[k]
    slots = buf.shape[0]
    if with_meta:
        ids = info[0, 0]
        r = info[0, 1]
        hi = r.astype(BF16).astype(F32)
        mid = (r - hi).astype(BF16).astype(F32)
        lo = r - hi - mid
        none = jnp.zeros_like(r)
        for i, pair in enumerate(((hi, mid), (lo, none), (ids, ids), (ids, none))):
            meta[i * 16:(i + 1) * 16, :] = jnp.concatenate(pair, axis=0).astype(BF16)
        meta[64:META, :] = jnp.zeros((META - 64, meta.shape[1]), BF16)

    def wait(slot):
        pltpu.make_async_copy(buf.at[slot], g_out.at[pl.ds(0, SRC_BLK)], sem.at[slot]).wait()

    def block(b, _):
        slot = lax.rem(done + b, slots)
        first = k * nsub_max + b * (SRC_BLK // SUB)
        build_onehot(oh, pos, subexp, sublocal, first)

        @pl.when(done + b >= slots)
        def _():
            wait(slot)

        col = 0
        for ref in (own, oth):
            w = ref.shape[1]
            buf[slot, :, col:col + w] = jnp.dot(oh[...], ref[...], preferred_element_type=F32).astype(BF16)
            col += w
        if with_meta:
            buf[slot, :, col:col + META] = nt_dot(oh[...], meta[...]).astype(BF16)
        for sub in range(SRC_BLK // SUB):
            dst = pl.multiple_of(subdst[first + sub], SUB)
            pltpu.make_async_copy(buf.at[slot, pl.ds(sub * SUB, SUB)], g_out.at[pl.ds(dst, SUB)], sem.at[slot]).start()
        return 0

    lax.fori_loop(0, n, block, 0)

    @pl.when(k == last)
    def _():
        for slot in range(slots):
            @pl.when(done + n > slot)
            def _():
                wait(slot)


def gather_call(t, half, rows_all, info, with_meta):
    n_src, _, n_tok = t["pos"].shape
    nsub_max = t["subexp"].shape[0] // n_src
    dh = rows_all.shape[1] // 2
    width = 2 * dh + (META if with_meta else 0)
    own = pl.BlockSpec((n_tok, dh), lambda s, *p: (s, p[5][0]))
    oth = pl.BlockSpec((n_tok, dh), lambda s, *p: (s, 1 - p[5][0]))
    return pl.pallas_call(
        functools.partial(gather_kernel, nsub_max, with_meta),
        out_shape=jax.ShapeDtypeStruct((t["rows"] + SRC_BLK, width), BF16),
        grid_spec=pltpu.PrefetchScalarGridSpec(
            num_scalar_prefetch=6, grid=(n_src,),
            in_specs=[own, oth,
                      pl.BlockSpec((1,) + info.shape[1:], lambda s, *p: (s, 0, 0, 0)),
                      pl.BlockSpec((1,) + t["pos"].shape[1:], lambda s, *p: (s, 0, 0))],
            out_specs=HBM,
            scratch_shapes=[pltpu.VMEM((SRC_BLK, n_tok), BF16), pltpu.VMEM((META, n_tok), BF16),
                            pltpu.VMEM((3, SRC_BLK, width), BF16), pltpu.SemaphoreType.DMA((3,))]),
        cost_estimate=pl.CostEstimate(flops=int(20e9), bytes_accessed=int(30e6), transcendentals=0),
        name="gather_rows",
    )(t["nblk"], t["blk_before"], t["subexp"], t["sublocal"], t["subdst"], half, rows_all, rows_all, info, t["pos"])


def expert_kernel(e0, accumulate, chained, blk_end, exp_rows, first_expert, x_hbm, dy_hbm, w1o, w1p, w3o, w3p, w2o, w2p, *refs):
    refs = refs[1 if chained else 0:]
    if accumulate:
        dw1_in, dw3_in, dw2_in = refs[:3]
    refs = refs[3 if chained or accumulate else 0:]
    dx_hbm, dw1, dw3, dw2, w13, w2, xbuf, dybuf, dxbuf, xsem, dysem, dxsem = refs
    e = e0 + pl.program_id(0)
    last = e0 + pl.num_programs(0) - 1
    dh = w1o.shape[1]
    d = 2 * dh
    f = w1o.shape[2]
    total = blk_end[last]
    start = blk_end[e0 - 1] if e0 else 0
    begin = jnp.where(e == 0, 0, blk_end[jnp.maximum(e - 1, 0)])
    end = blk_end[e]

    def fetch(b):
        src = pl.multiple_of(b * EXP_BLK, EXP_BLK)
        slot = lax.rem(b, 3)
        return (pltpu.make_async_copy(x_hbm.at[pl.ds(src, EXP_BLK)], xbuf.at[slot], xsem.at[slot]),
                pltpu.make_async_copy(dy_hbm.at[pl.ds(src, EXP_BLK)], dybuf.at[slot], dysem.at[slot]))

    def store(b):
        dst = pl.multiple_of(b * EXP_BLK, EXP_BLK)
        slot = lax.rem(b, 3)
        return pltpu.make_async_copy(dxbuf.at[slot], dx_hbm.at[pl.ds(dst, EXP_BLK)], dxsem.at[slot])

    @pl.when(e == e0)
    def _():
        for copy in fetch(start) + fetch(start + 1):
            copy.start()

    w13[0:dh, 0:f] = w1o[0]
    w13[dh:d, 0:f] = w1p[0]
    w13[0:dh, f:2 * f] = w3o[0]
    w13[dh:d, f:2 * f] = w3p[0]
    w2[:, 0:dh] = w2o[0]
    w2[:, dh:d] = w2p[0]
    if accumulate:
        dw1[...] = dw1_in[...]
        dw3[...] = dw3_in[...]
        dw2[...] = dw2_in[...]
    else:
        dw1[...] = jnp.zeros_like(dw1)
        dw3[...] = jnp.zeros_like(dw3)
        dw2[...] = jnp.zeros_like(dw2)

    def block(b, _):
        slot = lax.rem(b, 3)

        @pl.when(b + 2 < total)
        def _():
            for copy in fetch(b + 2):
                copy.start()

        for copy in fetch(b):
            copy.wait()

        @pl.when(b >= start + 3)
        def _():
            store(b - 3).wait()

        g = xbuf.at[slot]
        gy = dybuf.at[slot]
        dx = dxbuf.at[slot]
        live = jnp.minimum((exp_rows[e] - (b - begin) * EXP_BLK) // SUB, EXP_BLK // SUB)

        def clear(j, _):
            at = pl.ds(pl.multiple_of(j * SUB, SUB), SUB)
            g[at, :] = jnp.zeros((SUB, g.shape[1]), BF16)
            gy[at, :] = jnp.zeros((SUB, d), BF16)
            return 0

        lax.fori_loop(live, EXP_BLK // SUB, clear, 0)

        x = g[:, 0:d]
        meta = g[:, d:d + META].astype(F32)
        lane = lax.broadcasted_iota(jnp.int32, meta.shape, 1)
        ids = pltpu.roll(meta, META - 32, 1)
        mine = (ids == (first_expert[0] + e).astype(F32)) & (lane < 24)

        def piece(c):
            return jnp.sum(jnp.where(mine & (lane >= 8 * c) & (lane < 8 * c + 8), meta, 0.0), axis=1, keepdims=True)

        r = piece(0) + piece(1) + piece(2)
        dy32 = gy[...].astype(F32)
        scaled = (r * dy32).astype(BF16)
        h = jnp.dot(x, w13[...], preferred_element_type=F32)
        h1 = h[:, :f]
        h3 = h[:, f:]
        sig = jax.nn.sigmoid(h1)
        act = ((h1 * sig) * h3).astype(BF16)
        y = jnp.dot(act, w2[:, 0:dh], preferred_element_type=F32)
        dr = jnp.sum(dy32[:, 0:dh] * y, axis=1, keepdims=True)
        da = nt_dot(scaled, w2[...])
        dh1 = (da * h3 * sig * (1.0 + h1 * (1.0 - sig))).astype(BF16)
        dh3 = (da * h1 * sig).astype(BF16)
        dx[:, 0:dh] = (nt_dot(dh1, w1o[0]) + nt_dot(dh3, w3o[0])).astype(BF16)
        hi = dr.astype(BF16).astype(F32)
        mid = (dr - hi).astype(BF16).astype(F32)
        lo = dr - hi - mid
        spread = jnp.where(lane < 8, hi, jnp.where(lane < 16, mid, lo))
        dx[:, dh:dh + META] = jnp.where(mine, spread, 0.0).astype(BF16)
        store(b).start()
        dw1[0] += tn_dot(x[:, 0:dh], dh1)
        dw3[0] += tn_dot(x[:, 0:dh], dh3)
        dw2[0] += tn_dot(act, scaled[:, 0:dh])
        return 0

    lax.fori_loop(begin, end, block, 0)

    @pl.when(e == last)
    def _():
        store(total - 1).wait()
        store(total - 2).wait()
        store(total - 3).wait()


def expert_call(t, e0, first_expert, gx, gy, w_own, w_oth, dx_prev, dw_prev, accumulate):
    n_all, dh, f = w_own[0].shape
    n = w_oth[0].shape[0]
    wspec = pl.BlockSpec((1, dh, f), lambda e, *p: (e0 + e, 0, 0))
    dspec = pl.BlockSpec((1, f, dh), lambda e, *p: (e0 + e, 0, 0))
    wpart = pl.BlockSpec((1, dh, f), lambda e, *p: (e, 0, 0))
    dpart = pl.BlockSpec((1, f, dh), lambda e, *p: (e, 0, 0))
    in_specs = [HBM, HBM, wspec, wpart, wspec, wpart, dspec, dpart]
    args = [t["blk_end"], t["exp_rows"], first_expert, gx, gy, w_own[0], w_oth[0], w_own[1], w_oth[1], w_own[2], w_oth[2]]
    alias = {}
    if dx_prev is not None:
        alias[len(args)] = 0
        in_specs.append(HBM)
        args.append(dx_prev)
    if dw_prev is not None:
        for i, (w, spec) in enumerate(zip(dw_prev, (wspec, wspec, dspec))):
            alias[len(args)] = 1 + i
            in_specs.append(spec if accumulate else HBM)
            args.append(w)
    out = pl.pallas_call(
        functools.partial(expert_kernel, e0, accumulate, dx_prev is not None),
        out_shape=(jax.ShapeDtypeStruct((t["rows"], dh + META), BF16),
                   jax.ShapeDtypeStruct((n_all, dh, f), F32), jax.ShapeDtypeStruct((n_all, dh, f), F32),
                   jax.ShapeDtypeStruct((n_all, f, dh), F32)),
        grid_spec=pltpu.PrefetchScalarGridSpec(
            num_scalar_prefetch=3, grid=(n,), in_specs=in_specs, out_specs=[HBM, wspec, wspec, dspec],
            scratch_shapes=[pltpu.VMEM((2 * dh, 2 * f), BF16), pltpu.VMEM((f, 2 * dh), BF16),
                            pltpu.VMEM((3, EXP_BLK, 2 * dh + META), BF16), pltpu.VMEM((3, EXP_BLK, 2 * dh), BF16),
                            pltpu.VMEM((3, EXP_BLK, dh + META), BF16), pltpu.SemaphoreType.DMA((3,)),
                            pltpu.SemaphoreType.DMA((3,)), pltpu.SemaphoreType.DMA((3,))]),
        input_output_aliases=alias,
        cost_estimate=pl.CostEstimate(flops=int(20e9), bytes_accessed=int(60e6), transcendentals=0),
        name="expert_backward",
    )(*args)
    return out[0], out[1:]


def scatter_kernel(nsub_max, dh, nblk, subexp, sublocal, subsrc, pos, dx_hbm, out, oh, buf, acc, sem):
    k = pl.program_id(0)
    last = pl.num_programs(0) - 1
    n = nblk[k]
    side = lax.rem(k, 2)

    def fetch(src, to):
        def block(b, _):
            first = src * nsub_max + b * (SRC_BLK // SUB)
            for sub in range(SRC_BLK // SUB):
                row = pl.multiple_of(subsrc[first + sub], SUB)
                pltpu.make_async_copy(dx_hbm.at[pl.ds(row, SUB)], buf.at[to, b, pl.ds(sub * SUB, SUB)],
                                      sem.at[to, b]).start()
            return 0

        lax.fori_loop(0, nblk[src], block, 0)

    @pl.when(k == 0)
    def _():
        fetch(0, 0)

    @pl.when(k < last)
    def _():
        fetch(k + 1, 1 - side)

    acc[...] = jnp.zeros_like(acc)

    def block(b, _):
        build_onehot(oh, pos, subexp, sublocal, k * nsub_max + b * (SRC_BLK // SUB))
        pltpu.make_async_copy(dx_hbm.at[pl.ds(0, SRC_BLK)], buf.at[side, b], sem.at[side, b]).wait()
        acc[...] += tn_dot(buf[side, b, :, 0:dh + 32], oh[...])
        return 0

    lax.fori_loop(0, n, block, 0)
    out[0, 0:dh, :] = acc[0:dh, :]
    out[0, dh:dh + 8, :] = acc[dh:dh + 8, :] + acc[dh + 8:dh + 16, :] + acc[dh + 16:dh + 24, :]


def scatter_call(t, dx_rows):
    n_src, _, n_tok = t["pos"].shape
    dh = dx_rows.shape[1] - META
    nsub_max = t["subexp"].shape[0] // n_src
    most = nsub_max // (SRC_BLK // SUB)
    return pl.pallas_call(
        functools.partial(scatter_kernel, nsub_max, dh),
        out_shape=jax.ShapeDtypeStruct((n_src, dh + 8, n_tok), F32),
        grid_spec=pltpu.PrefetchScalarGridSpec(
            num_scalar_prefetch=4, grid=(n_src,),
            in_specs=[pl.BlockSpec((1,) + t["pos"].shape[1:], lambda s, *p: (s, 0, 0)), HBM],
            out_specs=pl.BlockSpec((1, dh + 8, n_tok), lambda s, *p: (s, 0, 0)),
            scratch_shapes=[pltpu.VMEM((SRC_BLK, n_tok), BF16), pltpu.VMEM((2, most, SRC_BLK, dh + META), BF16),
                            pltpu.VMEM((dh + 32, n_tok), F32), pltpu.SemaphoreType.DMA((2, most))]),
        cost_estimate=pl.CostEstimate(flops=int(10e9), bytes_accessed=int(30e6), transcendentals=0),
        name="scatter_rows",
    )(t["nblk"], t["subexp"], t["sublocal"], t["subsrc"], t["pos"], dx_rows)


def routing_tables(ids, first_expert, n_exp, capacity):
    n_src, _, n_tok = ids.shape
    eid = first_expert.astype(F32) + jnp.arange(n_exp, dtype=F32)
    mask = jnp.any(ids[:, None, :, :] == eid[None, :, None, None], axis=2)
    upper = (jnp.arange(n_tok)[:, None] < jnp.arange(n_tok)[None, :]).astype(BF16)
    before = jnp.dot(mask.reshape(n_src * n_exp, n_tok).astype(BF16), upper, preferred_element_type=F32)
    before = before.reshape(n_src, n_exp, n_tok)
    kept = mask & (before < capacity)
    pos = jnp.where(kept, before, -1024.0)[:, :, None, :] - jnp.arange(SUB, dtype=F32)[None, None, :, None]
    pos = jnp.where(pos < -500.0, -512.0, pos).astype(BF16).reshape(n_src, n_exp * SUB, n_tok)
    cnt = jnp.sum(kept.astype(jnp.int32), axis=2)
    per_src = SRC_BLK // SUB
    per_exp = EXP_BLK // SUB
    subs = (cnt + SUB - 1) // SUB
    cap_subs = -(-capacity // SUB)
    nsub_max = -(-n_exp * cap_subs // per_src) * per_src
    src_end = jnp.cumsum(subs, axis=1)
    src_off = src_end - subs
    nsub = src_end[:, -1]
    exp_subs = jnp.sum(subs, axis=0)
    exp_blocks = jnp.maximum(1, -(-exp_subs // per_exp))
    blk_end = jnp.cumsum(exp_blocks)
    blk_off = blk_end - exp_blocks
    seg_off = blk_off[None, :] * per_exp + jnp.cumsum(subs, axis=0) - subs
    q = jnp.arange(nsub_max, dtype=jnp.int32)
    subexp = jnp.minimum(jnp.sum((src_end[:, None, :] <= q[None, :, None]).astype(jnp.int32), axis=2), n_exp - 1)
    pick = subexp[:, :, None] == jnp.arange(n_exp)[None, None, :]
    rel = q[None, :] - jnp.sum(jnp.where(pick, src_off[:, None, :], 0), axis=2)
    live = q[None, :] < nsub[:, None]
    seg = jnp.sum(jnp.where(pick, seg_off[:, None, :], 0), axis=2) + rel
    rows = n_exp * max(1, -(-n_src * cap_subs // per_exp)) * EXP_BLK
    spare = rows + (q % per_src)[None, :] * SUB
    nblk = -(-nsub // per_src)
    return dict(
        pos=pos, nblk=nblk, blk_before=jnp.cumsum(nblk) - nblk, subexp=subexp.reshape(-1),
        sublocal=jnp.where(live, rel * SUB, 1 << 20).reshape(-1),
        subdst=jnp.where(live, seg * SUB, spare).reshape(-1), subsrc=jnp.where(live, seg * SUB, 0).reshape(-1),
        blk_end=blk_end, exp_rows=exp_subs * SUB, rows=rows)


def gather_by_doubling(v, axis, n):
    me = lax.axis_index(axis)
    v = v[None]
    step = 1
    while step < n:
        got = lax.ppermute(v, axis, [(i, i ^ step) for i in range(n)])
        upper = (me // step) % 2 == 1
        v = jnp.concatenate([jnp.where(upper, got, v), jnp.where(upper, v, got)])
        step *= 2
    return v


def solution(mesh):
    n_ep = mesh.shape["ep"]
    tok_spec = P(("fsdp", "ep"), None)
    spec_in = P("ep", "fsdp", None)
    spec_out = P("ep", None, "fsdp")
    swap = [(0, 1), (1, 0)]

    def layer(x_tok, dy_tok, expert_ids, route_w, w_gate, w_up, w_down):
        tok_dev, top_k = expert_ids.shape
        exp_local = w_gate.shape[0]
        dh = w_gate.shape[1]
        capacity = capacity_of(tok_dev, top_k, exp_local * n_ep)
        me = lax.axis_index("fsdp")
        pad = ((0, 8 - top_k), (0, 0))
        info = jnp.stack([jnp.pad(expert_ids.T.astype(F32), pad, constant_values=-1.0),
                          jnp.pad(route_w.T, pad)])
        w_own = (w_gate, w_up, w_down)
        cut = (exp_local * 7) // 10
        x_a = lax.all_gather(x_tok, "ep", axis=0, tiled=True)
        info = jnp.stack([info, lax.ppermute(info, "fsdp", swap)])
        info = gather_by_doubling(info, "ep", n_ep)
        info_a = info[:, 0]
        info_b = info[:, 1]
        x_z = lax.ppermute(x_tok, "fsdp", swap)
        dy_z = lax.ppermute(dy_tok, "fsdp", swap)
        w_lo = tuple(lax.ppermute(w[:cut], "fsdp", swap) for w in w_own)
        w_hi = tuple(lax.ppermute(w[cut:], "fsdp", swap) for w in w_own)
        first_expert = lax.axis_index("ep") * exp_local
        t_b = routing_tables(info_b[:, 0], first_expert, exp_local, capacity)
        t_a = routing_tables(info_a[:, 0], first_expert, exp_local, capacity)
        rows = t_a.pop("rows"), t_b.pop("rows")
        x_z, t_a, t_b = lax.optimization_barrier((x_z, t_a, t_b))
        t_a["rows"], t_b["rows"] = rows
        x_b = lax.all_gather(x_z, "ep", axis=0, tiled=True)
        dy_b = lax.all_gather(dy_z, "ep", axis=0, tiled=True)
        dy_a = lax.all_gather(dy_tok, "ep", axis=0, tiled=True)

        half = me.reshape(1)
        first = first_expert.reshape(1)
        gx_a = gather_call(t_a, half, x_a, info_a, True)
        gx_b = gather_call(t_b, half, x_b, info_b, True)
        gx_a, gx_b, dy_b = lax.optimization_barrier((gx_a, gx_b, dy_b))
        gy_b = gather_call(t_b, half, dy_b, info_b, False)
        gy_a = gather_call(t_a, half, dy_a, info_a, False)
        dx_b, dw = expert_call(t_b, 0, first, gx_b, gy_b, w_own, w_lo, None, None, False)
        dx_b, dw = expert_call(t_b, cut, first, gx_b, gy_b, w_own, w_hi, dx_b, dw, False)
        out_b = scatter_call(t_b, dx_b)
        sum_b = lax.psum_scatter(out_b, "ep", scatter_dimension=0, tiled=False)
        dx_a, dw = expert_call(t_a, 0, first, gx_a, gy_a, w_own, w_lo, None, dw, True)
        dx_a, dw = expert_call(t_a, cut, first, gx_a, gy_a, w_own, w_hi, dx_a, dw, True)
        out_a = scatter_call(t_a, dx_a)
        sum_a = lax.psum_scatter(out_a, "ep", scatter_dimension=0, tiled=False)
        dx_other = lax.ppermute(sum_b[:dh].astype(BF16), "fsdp", swap)
        dr_other = lax.ppermute(sum_b[dh:], "fsdp", swap)
        dx_mine = sum_a[:dh].astype(BF16)
        grad_x = jnp.where(me == 0, jnp.concatenate([dx_mine, dx_other]), jnp.concatenate([dx_other, dx_mine])).T
        route_grad = (sum_a[dh:] + dr_other)[:top_k].T
        return grad_x, route_grad, dw[0], dw[1], dw[2]

    return jax.shard_map(
        layer, mesh=mesh,
        in_specs=(tok_spec, tok_spec, tok_spec, tok_spec, spec_in, spec_in, spec_out),
        out_specs=(tok_spec, tok_spec, spec_in, spec_in, spec_out),
        check_vma=False)
```
